512 devices in a mesh: seq: 128 (over z, y, core), rep: 4 (over x).
Axes of the slice: x: 4, y: 4, z: 16, core: 2. Of those that a mesh axis runs over, the one named last changes fastest.
Arguments:
- queries: bfloat16 [512, 32, 128], P('seq', 'rep'), may hold values from -48 to 48
- key_cache: bfloat16 [8, 262144, 128], P('rep', 'seq'), may hold values from -6 to 6
- value_cache: bfloat16 [8, 262144, 128], P('rep', 'seq'), may hold values from -6 to 6
- summary_keys: bfloat16 [8, 128, 128], P('rep', 'seq'), may hold values from -16 to 16
- summary_values: bfloat16 [8, 128, 128], P('rep', 'seq'), may hold values from -6 to 6
- owner_map: int32 [128], replicated, may hold values from 0 to 127, each once
- super_ids: int32 [512, 8, 4], P(None, 'rep'), may hold values from 0 to 127, as said below
- fine_ids: int32 [512, 8, 16], P(None, 'rep'), may hold values from 0 to 63, all different within a row
Outputs:
- attended: bfloat16 [512, 32, 128], P(('seq', 'rep'))
The draws below stay inside these ranges and needn't reach their ends.
Inputs may be any that keep to these rules, and one draw needn't show every extreme that they name: `super_ids`: each row names 4 different super-blocks; among the rows of one sender group (the 4 requests of one index of seq with the 2 key-value heads of one index of rep) no super-block is named more than 2 times, and in every such group some super-block is named exactly 2 times. `fine_ids`: each row names 16 different positions; position p is block p % 16 of super-block super_ids[r, g, p // 16]. `owner_map`: a permutation; slot q covers fine blocks q * 16 to q * 16 + 15 of the caches.
All inputs are finite; a program needn't handle non-finite values.
Results may differ from the reference program's by a relative error of at most 0.004.
Values may be sent and summed in bfloat16 or wider, within the bound.
A program may use at most 64 MiB of HBM per device.

```python
import math
import jax
import jax.numpy as jnp
from jax import lax

H = 32
KVH = 8
HD = 128
BLK = 128
SUPER = 16
REQ_DEV = 4
NSEL_SB = 4
NSEL_FB = 16
KVH_DEV = 2
NTOK = 262144
NSB = 128
REQUESTS = 512
CAP = 2


def draw_queries(key, part):
    random_part = jnp.clip(jax.random.normal(jax.random.fold_in(key, 11), (REQUESTS, H, HD), jnp.float32), -5.0, 5.0)
    return (3.0 * random_part).astype(jnp.bfloat16)


def draw_summary_keys(key, part):
    random_part = jnp.clip(jax.random.normal(jax.random.fold_in(key, 21), (KVH, NSB, HD), jnp.float32), -5.0, 5.0)
    return random_part.astype(jnp.bfloat16)


def draw_super_ids(key, part):
    seq_count = REQUESTS // REQ_DEV
    rep_count = KVH // KVH_DEV
    senders = seq_count * rep_count
    group_rows = REQ_DEV * KVH_DEV
    others = NSB - 1
    hottest = jax.random.randint(jax.random.fold_in(key, 31), (), 0, NSB)
    order_keys = jax.random.split(jax.random.fold_in(key, 32), senders)
    orders = jax.vmap(lambda single: jax.random.permutation(single, others))(order_keys)
    rank_keys = jax.random.split(jax.random.fold_in(key, 33), senders)
    row_rank = jax.vmap(lambda single: jax.random.permutation(single, group_rows))(rank_keys)
    position = (jnp.arange(group_rows)[:, None] * NSEL_SB + jnp.arange(NSEL_SB)[None, :]) % others
    picks = orders[:, position.reshape(-1)].reshape(senders, group_rows, NSEL_SB)
    picks = picks + (picks >= hottest).astype(picks.dtype)
    first = jnp.where(row_rank < CAP, hottest, picks[:, :, 0])
    picks = jnp.concatenate([first[:, :, None], picks[:, :, 1:]], axis=2)
    picks = picks.reshape(seq_count, rep_count, REQ_DEV, KVH_DEV, NSEL_SB)
    picks = jnp.transpose(picks, (0, 2, 1, 3, 4)).reshape(REQUESTS, KVH, NSEL_SB)
    return picks.astype(jnp.int32)


def block_scale(own_key, shape, shards, least, high):
    factor_of = 1.0
    for axis_at, blocks in shards:
        draws = jax.random.uniform(jax.random.fold_in(jax.random.fold_in(own_key, 6), axis_at), (blocks,), jnp.float32, least / len(shards), high / len(shards))
        factor_of = factor_of * jnp.repeat(jnp.exp(draws), shape[axis_at] // blocks).reshape((-1,) + (1,) * (len(shape) - 1 - axis_at))
    return factor_of


def different_ones(rng, rows, number_of, top, lift):
    ranking = jax.random.permutation(jax.random.fold_in(rng, 1), number_of)
    boost = ranking
    for power in range(3):
        boost = boost * boost // number_of
    boost = boost * lift // number_of
    tickets = jax.random.randint(jax.random.fold_in(rng, 2), (rows, number_of), 0, 4096) + boost
    fixed_rows = jax.random.permutation(jax.random.fold_in(rng, 3), rows)[jnp.arange(number_of) % rows]
    tickets = jnp.where(jnp.arange(rows)[:, None] == fixed_rows[None, :], 1 << 14, tickets)
    score = tickets * number_of + jnp.arange(number_of)
    return lax.top_k(score.astype(jnp.int32), top)[1].astype(jnp.int32)


def normal_values(own_key, dims, scale, limit, cuts=(), kind=jnp.bfloat16):
    drawn = jax.random.normal(own_key, dims, jnp.float32) * scale
    if len(cuts) > 0:
        drawn = block_scale(own_key, dims, cuts, -0.22, 0.18) * drawn
    return jnp.clip(drawn, min=-limit, max=limit).astype(kind)


def setup_inputs(seed: int = 0) -> dict:
    arg_keys = jax.random.split(jax.random.key(seed), 9)
    return {
        "queries": draw_queries(jax.random.fold_in(arg_keys[8], 71), 0),
        "key_cache": normal_values(arg_keys[1], (KVH, NTOK, HD), 1.0, 6.0, ((0, 4), (1, 128))),
        "value_cache": normal_values(arg_keys[2], (KVH, NTOK, HD), 1.0, 6.0, ((0, 4), (1, 128))),
        "summary_keys": draw_summary_keys(jax.random.fold_in(arg_keys[8], 71), 0),
        "summary_values": normal_values(arg_keys[4], (KVH, NSB, HD), 1.0, 6.0, ((0, 4), (1, 128))),
        "owner_map": jax.random.permutation(arg_keys[5], NSB).astype(jnp.int32),
        "super_ids": draw_super_ids(jax.random.fold_in(arg_keys[8], 71), 0),
        "fine_ids": different_ones(arg_keys[7], REQUESTS * KVH, NSEL_SB * SUPER, NSEL_FB, 2048).reshape((REQUESTS, KVH, NSEL_FB)),
    }


NEGATIVE = -1.0e30


def reference(queries, key_cache, value_cache, summary_keys, summary_values, owner_map, super_ids, fine_ids):
    kv_heads = key_cache.shape[0]
    head_dim = queries.shape[2]
    per_group = queries.shape[1] // kv_heads
    scaling = head_dim ** -0.5
    slots = owner_map[super_ids]
    picked = jnp.take_along_axis(slots, (fine_ids // SUPER).astype(jnp.int32), axis=2)
    chosen = (picked * SUPER + fine_ids % SUPER).astype(jnp.int32)
    key_blocks = key_cache.reshape(kv_heads, -1, BLK, head_dim)
    value_blocks = value_cache.reshape(kv_heads, -1, BLK, head_dim)
    slot_count = summary_keys.shape[1]
    head_index = jnp.arange(kv_heads, dtype=jnp.int32)[:, None]
    wide_keys = summary_keys.astype(jnp.float32)
    wide_values = summary_values.astype(jnp.float32)

    def attend(pieces):
        query, picked_blocks, picked_slots = pieces
        grouped = query.astype(jnp.float32).reshape(kv_heads, per_group, head_dim)
        fine_keys = key_blocks[head_index, picked_blocks].astype(jnp.float32).reshape(kv_heads, -1, head_dim)
        fine_values = value_blocks[head_index, picked_blocks].astype(jnp.float32).reshape(kv_heads, -1, head_dim)
        fine_scores = jnp.einsum("gqd,gtd->gqt", grouped, fine_keys, precision=lax.Precision.HIGHEST) * scaling
        kept = jnp.logical_not(jnp.any(picked_slots[:, :, None] == jnp.arange(slot_count, dtype=jnp.int32)[None, None, :], axis=1))
        coarse_scores = jnp.einsum("gqd,gsd->gqs", grouped, wide_keys, precision=lax.Precision.HIGHEST) * scaling + math.log(SUPER)
        coarse_scores = jnp.where(kept[:, None, :], coarse_scores, NEGATIVE)
        every_score = jnp.concatenate([fine_scores, coarse_scores], axis=2)
        highest = jnp.max(every_score, axis=2, keepdims=True)
        weights = jnp.exp(every_score - highest)
        joined_values = jnp.concatenate([fine_values, wide_values], axis=1)
        result = jnp.einsum("gqn,gnd->gqd", weights, joined_values, precision=lax.Precision.HIGHEST)
        result = result / jnp.sum(weights, axis=2)[..., None]
        return result.reshape(-1, head_dim).astype(jnp.bfloat16)

    return lax.map(attend, (queries, chosen, slots))
```

```python
import functools
import math

import jax
import jax.numpy as jnp
from jax import lax
from jax.experimental import pallas as pl
from jax.experimental.pallas import tpu as pltpu
from jax.sharding import PartitionSpec as P

MESH = pl.DeviceIdType.MESH
F32, BF16, I32 = jnp.float32, jnp.bfloat16, jnp.int32
NZ, NP, NY, NX = 16, 8, 4, 4
HD, BLK, SUPER, NSEL, NFINE = 128, 128, 16, 4, 16
NREQ, SPAN = 512, 2048
NEG = -1e30
SCALE2 = HD**-0.5 / math.log(2.0)
Z_ORDER = (8, 7, 9, 6, 10, 5, 11, 4, 12, 3, 13, 2, 14, 1, 15)


def iota(shape, dim):
    return lax.broadcasted_iota(I32, shape, dim)


def dot(a, b, dims=((1,), (0,))):
    return lax.dot_general(a, b, (dims, ((), ())), preferred_element_type=F32)


def group_rank(hits):
    i = jnp.bitwise_and(iota(hits[0].shape, 1), 3)
    before, total = [], []
    for h in hits:
        b = jnp.zeros_like(h)
        t = h
        for d in (1, 2, 3):
            b = b + jnp.where(i >= d, pltpu.roll(h, d, 1), 0)
            t = t + jnp.where(i + d <= 3, pltpu.roll(h, NREQ - d, 1), 0)
        before.append(b)
        total.append(t + b)
    return before[0], before[1] + total[0]


def kernel(
    q_h, kc_h, vc_h, sk_h, sv_h, om_h, si_h, fi_h, o_ref,
    sk, sv, om, si, fi, kcat, vcat, v_t, qz, qs, rq, rsel, meta, s_s, p_s,
    os_, ol, ro, rl, pzs, lzs, pz, lz, sz, szf, sf, xs,
    load_sem, kv_sem, q1s, q1r, q2s, q2r, r1s, r1r, l1s, l1r, r2s, r2r, l2s, l2r, szs, szr, sfs, sfr, xss, xsr, loc,
):
    me, rep = lax.axis_index("seq"), lax.axis_index("rep")
    z, p = me // NP, lax.rem(me, NP)
    y, c = p // 2, lax.rem(p, 2)

    def z_peer(d):
        return lax.rem(z + d, NZ)

    def plane_peer(dy, dc):
        return lax.rem(y + dy, NY) * 2 + lax.rem(c + dc, 2)

    plane = [(dy, dc) for dy in (2, 1, 3, 0) for dc in (0, 1) if dy or dc]

    barrier = pltpu.get_barrier_semaphore()
    for d in Z_ORDER:
        pl.semaphore_signal(barrier, inc=1, device_id=(z_peer(d) * NP + p, rep), device_id_type=MESH)
    for dy, dc in plane:
        pl.semaphore_signal(barrier, inc=1, device_id=(z * NP + plane_peer(dy, dc), rep), device_id_type=MESH)
    for d in range(1, NX):
        pl.semaphore_signal(barrier, inc=1, device_id=(me, lax.rem(rep + d, NX)), device_id_type=MESH)

    def remote(src, dst, ss, rs, seq, x=None):
        return pltpu.make_async_remote_copy(
            src_ref=src, dst_ref=dst, send_sem=ss, recv_sem=rs,
            device_id=(seq, rep if x is None else x), device_id_type=MESH,
        )

    def wait(ref, sem):
        pltpu.make_async_copy(ref, ref, sem).wait()

    loads = [
        pltpu.make_async_copy(a, b, load_sem.at[n])
        for n, (a, b) in enumerate([(q_h, qz.at[z]), (sk_h, sk), (sv_h, sv), (om_h, om), (si_h, si), (fi_h, fi)])
    ]
    kv_loads = [
        pltpu.make_async_copy(a.at[g], b.at[:, pl.ds(g * HD, HD)], kv_sem.at[2 * n + g])
        for n, (a, b) in enumerate([(kc_h, kcat), (vc_h, vcat)])
        for g in (0, 1)
    ]
    for copy in loads + kv_loads:
        copy.start()
    for copy in loads:
        copy.wait()
    sz[z] = jnp.concatenate([sk[...].astype(F32), sv[...].astype(F32)], axis=0).astype(BF16)

    pl.semaphore_wait(barrier, len(Z_ORDER) + len(plane) + NX - 1)

    for d in Z_ORDER:
        remote(qz.at[z], qz.at[z], q1s, q1r, z_peer(d) * NP + p).start()
    for d in Z_ORDER:
        remote(sz.at[z], sz.at[z], szs, szr, z_peer(d) * NP + p).start()

    omv = om[...]
    siv = [[si[g, j : j + 1, :] for j in range(NSEL)] for g in (0, 1)]
    lane128 = iota((NP, 128), 1)
    sig8 = jnp.sum(jnp.where(omv == z * NP + iota((NP, 128), 0), lane128, 0), axis=1, keepdims=True)
    hits = []
    for g in (0, 1):
        h = siv[g][0] == sig8
        for j in range(1, NSEL):
            h = jnp.logical_or(h, siv[g][j] == sig8)
        hits.append(jnp.where(h, 1, 0))
    ranks = group_rank(hits)
    row, lane = iota((NREQ, NREQ), 0), iota((NREQ, NREQ), 1)
    source = (lane >> 5) * 32 + p * 4 + ((lane >> 3) & 3)
    picked = jnp.zeros((NP, NREQ), F32)
    for g in (0, 1):
        spread = jnp.where(row == jnp.where(((lane >> 2) & 1) == g, source, -1), 1.0, 0.0).astype(BF16)
        code = jnp.where(hits[g] > 0, ranks[g] + 1, 0).astype(F32).astype(BF16)
        picked = picked + dot(code, spread)
    rsel[...] = picked

    sig1 = jnp.sum(jnp.where(omv == me, lane128[0:1], 0), axis=1, keepdims=True)
    own_hits, own_bits = [], []
    for g in (0, 1):
        h, jsel = jnp.zeros((1, NREQ), I32), jnp.zeros((1, NREQ), I32)
        for j in range(NSEL):
            same = siv[g][j] == sig1
            h = jnp.where(same, 1, h)
            jsel = jnp.where(same, j, jsel)
        target = jsel * SUPER + iota((SUPER, NREQ), 0)
        bits = fi[g, 0:1, :] == target
        for k in range(1, NFINE):
            bits = jnp.logical_or(bits, fi[g, k : k + 1, :] == target)
        own_hits.append(jnp.broadcast_to(h, (8, NREQ)))
        own_bits.append(jnp.where(bits, 1.0, 0.0))
    own_ranks = group_rank(own_hits)
    sub8 = iota((8, NREQ), 0)
    stacked = []
    for slot in (0, 1):
        use = [jnp.where(jnp.logical_and(own_hits[g] > 0, own_ranks[g] == slot), 1.0, 0.0) for g in (0, 1)]
        wanted = own_bits[0] * use[0][0:1] + own_bits[1] * use[1][0:1]
        flags = jnp.where(sub8 == 0, use[0], jnp.where(sub8 == 1, use[1], 0.0))
        stacked.append(jnp.concatenate([wanted, flags, jnp.zeros((8, NREQ), F32)], axis=0).astype(BF16))
    for chunk in range(NY):
        row, col = iota((NREQ, 256), 0), iota((NREQ, 256), 1)
        sender = ((col >> 3) & 15) * NP + chunk * 2 + (col >> 7)
        acc = jnp.zeros((32, 256), F32)
        for slot in (0, 1):
            at = jnp.where(((col >> 2) & 1) == slot, sender, -1)
            acc = acc + dot(stacked[slot], jnp.where((row >> 2) == at, 1.0, 0.0).astype(BF16))
        meta[chunk] = acc

    srow, slane = iota((128, NREQ), 0), iota((128, NREQ), 1)
    base = jnp.where(
        jnp.logical_and((srow >> 3) == (slane >> 5), (srow & 3) == (slane & 3)), ((srow >> 2) & 1) + 1, -1
    ).astype(F32)

    wait(qz.at[pl.ds(0, NZ - 1)], q1r)
    every = qz[...].reshape(NREQ, HD)
    for dy, dc in [(0, 0)] + plane:
        peer = plane_peer(dy, dc)
        choose = jnp.where(base == rsel[pl.ds(peer, 1), :], 1.0, 0.0).astype(BF16)
        qs[peer] = dot(choose, every).astype(BF16)
        if dy or dc:
            remote(qs.at[peer], rq.at[p], q2s, q2r.at[dy], z * NP + peer).start()
        else:
            pltpu.make_async_copy(qs.at[peer], rq.at[peer], loc.at[0]).start()

    wait(sz.at[pl.ds(0, NZ - 1)], szr)
    for n in range(NZ):
        szf[n * 4 : n * 4 + 4, :] = sz[n].astype(F32)
    sf[p] = szf[...].astype(BF16)
    for dy, dc in plane:
        remote(sf.at[p], sf.at[p], sfs, sfr, z * NP + plane_peer(dy, dc)).start()

    for copy in kv_loads:
        copy.wait()
    v_t[...] = jnp.transpose(vcat[...], (1, 0))
    wait(qs.at[0], loc.at[0])

    def chunk_step(k, carry):
        @pl.when(k == 0)
        def _():
            wait(rq.at[0], q2r.at[0])

        @pl.when(k > 0)
        def _():
            wait(rq.at[pl.ds(0, 2)], q2r.at[k])

        yy = lax.rem(y + NY - k, NY)
        m_all = meta[yy]
        flags = jnp.transpose(m_all[16:24], (1, 0)).astype(BF16)
        rows = rq[pl.ds(yy * 2, 2)].reshape(256, HD)
        split = jnp.concatenate([rows * flags[:, 0:1], rows * flags[:, 1:2]], axis=1)
        s_s[...] = dot(kcat[...], split, ((1,), (1,)))
        bias = jnp.where(m_all[0:16] > 0.5, 0.0, NEG)
        peak = jnp.full((1, 256), -3e38, F32)
        for b in range(SUPER):
            top = jnp.max(s_s[b * BLK : (b + 1) * BLK, :], axis=0, keepdims=True)
            peak = jnp.maximum(peak, top + bias[b : b + 1])
        total = jnp.zeros((1, 256), F32)
        for b in range(SUPER):
            w = jnp.exp2((s_s[b * BLK : (b + 1) * BLK, :] + (bias[b : b + 1] - peak)) * SCALE2)
            total = total + jnp.sum(w, axis=0, keepdims=True)
            p_s[b * BLK : (b + 1) * BLK, :] = w.astype(BF16)
        out = dot(v_t[...], p_s[...])
        out = jnp.where(m_all[17:18] > 0.5, out[HD : 2 * HD], out[0:HD]) * (1.0 / total)
        log_sum = peak * SCALE2 + jnp.log2(total)
        for n in (0, 1):
            os_[yy * 2 + n] = out[:, n * 128 : (n + 1) * 128].astype(BF16)
            ol[yy * 2 + n] = log_sum[:, n * 128 : (n + 1) * 128]

        mine, other = yy * 2 + c, yy * 2 + 1 - c

        @pl.when(k == 0)
        def _():
            pltpu.make_async_copy(os_.at[mine], ro.at[mine], loc.at[1]).start()
            pltpu.make_async_copy(ol.at[mine], rl.at[mine], loc.at[2]).start()

        @pl.when(k > 0)
        def _():
            remote(os_.at[mine], ro.at[p], r1s, r1r, z * NP + mine).start()
            remote(ol.at[mine], rl.at[p], l1s, l1r, z * NP + mine).start()

        remote(os_.at[other], ro.at[p], r1s, r1r, z * NP + other).start()
        remote(ol.at[other], rl.at[p], l1s, l1r, z * NP + other).start()
        return carry

    lax.fori_loop(0, NY, chunk_step, 0)

    wait(sf.at[pl.ds(0, NP - 1)], sfr)
    every_summary = sf[...].reshape(NREQ, HD)
    erow, elane = iota((128, 128), 0), iota((128, 128), 1)
    om_col = jnp.sum(jnp.where(erow == elane, omv, 0), axis=1, keepdims=True)
    tok = iota((1, NREQ), 1)
    tok_slot = ((tok >> 2) & 15) * NP + (tok >> 6)
    tok_super = jnp.sum(jnp.where(om_col == tok_slot, iota((128, NREQ), 0), 0), axis=0, keepdims=True)
    r_head, r_tok = iota((32, NREQ), 0), iota((32, NREQ), 1)
    r_group = (r_head >> 2) & 1
    kept = (r_tok & 3) == r_group
    for j in range(NSEL):
        ids = jnp.where(r_group == 0, siv[0][j], siv[1][j])
        own = jnp.sum(jnp.where(r_tok == me * 4 + (r_head >> 3), ids, 0), axis=1, keepdims=True)
        kept = jnp.logical_and(kept, tok_super != own)
    c_score = dot(qz[z], every_summary, ((1,), (1,))) * SCALE2 + 4.0
    c_score = jnp.where(kept, c_score, NEG)
    c_peak = jnp.max(c_score, axis=1, keepdims=True)
    c_w = jnp.where(kept, jnp.exp2(c_score - c_peak), 0.0)
    c_sum = jnp.sum(c_w, axis=1, keepdims=True)
    c_out = dot(pltpu.roll(c_w, 2, 1).astype(BF16), every_summary)

    wait(os_.at[0], loc.at[1])
    wait(ol.at[0], loc.at[2])
    wait(ro.at[pl.ds(0, NP - 1)], r1r)
    wait(rl.at[pl.ds(0, NP - 1)], l1r)
    l_cols = jnp.transpose(rl[...].reshape(NP, 128), (1, 0))
    peak = jnp.full((1, NREQ), NEG, F32)
    for n in range(NP):
        lse = jnp.where(base == rsel[n : n + 1, :], l_cols[:, n : n + 1], NEG)
        peak = jnp.maximum(peak, jnp.max(lse, axis=0, keepdims=True))
    total = jnp.zeros((1, NREQ), F32)
    merged = jnp.zeros((HD, NREQ), F32)
    for n in range(NP):
        w = jnp.where(base == rsel[n : n + 1, :], jnp.exp2(l_cols[:, n : n + 1] - peak), 0.0)
        total = total + jnp.sum(w, axis=0, keepdims=True)
        merged = merged + dot(ro[n], w.astype(BF16))
    some = total > 0.0
    merged = merged * jnp.where(some, 1.0 / jnp.where(some, total, 1.0), 0.0)
    log_sum = jnp.where(some, peak + jnp.log2(jnp.where(some, total, 1.0)), NEG)
    pzs[...] = jnp.transpose(merged, (1, 0)).astype(BF16).reshape(NZ, 32, HD)
    for n in range(NZ):
        part = log_sum[:, (n // 4) * 128 : (n // 4) * 128 + 128]
        lzs[n] = pltpu.roll(part, 128 - 32 * (n % 4), 1) if n % 4 else part
    keep = [
        pltpu.make_async_copy(pzs.at[z], pz.at[z], loc.at[3]),
        pltpu.make_async_copy(lzs.at[z], lz.at[z], loc.at[4]),
    ]
    for copy in keep:
        copy.start()
    for d in Z_ORDER:
        zz = z_peer(d)
        remote(pzs.at[zz], pz.at[z], r2s, r2r, zz * NP + p).start()
        remote(lzs.at[zz], lz.at[z], l2s, l2r, zz * NP + p).start()
    for copy in keep:
        copy.wait()
    wait(pz.at[pl.ds(0, NZ - 1)], r2r)
    wait(lz.at[pl.ds(0, NZ - 1)], l2r)

    lse = jnp.transpose(lz[...].reshape(NZ, 128), (1, 0))[0:32]
    c_lse = c_peak + jnp.log2(c_sum)
    top = jnp.maximum(jnp.max(lse, axis=1, keepdims=True), c_lse)
    w = jnp.exp2(lse - top)
    c_scale = jnp.exp2(c_peak - top)
    total = jnp.sum(w, axis=1, keepdims=True) + c_scale * c_sum
    result = c_out * c_scale
    for n in range(NZ):
        result = result + pz[n].astype(F32) * w[:, n : n + 1]
    xs[...] = (result / total).astype(BF16).reshape(NX, 8, HD)
    keep = pltpu.make_async_copy(xs.at[rep], o_ref.at[rep], loc.at[5])
    keep.start()
    for d in range(1, NX):
        x = lax.rem(rep + d, NX)
        remote(xs.at[x], o_ref.at[rep], xss, xsr, me, x).start()

    wait(qz.at[pl.ds(0, NZ - 1)], q1s)
    wait(sz.at[pl.ds(0, NZ - 1)], szs)
    wait(qs.at[pl.ds(0, NP - 1)], q2s)
    wait(sf.at[pl.ds(0, NP - 1)], sfs)
    wait(os_.at[pl.ds(0, NP - 1)], r1s)
    wait(ol.at[pl.ds(0, NP - 1)], l1s)
    wait(pzs.at[pl.ds(0, NZ - 1)], r2s)
    wait(lzs.at[pl.ds(0, NZ - 1)], l2s)
    keep.wait()
    wait(xs.at[pl.ds(0, NX - 1)], xss)
    wait(o_ref.at[pl.ds(0, NX - 1)], xsr)


def shards(queries, key_cache, value_cache, summary_keys, summary_values, owner_map, super_ids, fine_ids):
    vmem, dma = pltpu.VMEM, pltpu.SemaphoreType.DMA
    out = pl.pallas_call(
        kernel,
        out_shape=jax.ShapeDtypeStruct((NX, 8, HD), BF16),
        in_specs=[pl.BlockSpec(memory_space=pltpu.HBM)] * 8,
        out_specs=pl.BlockSpec(memory_space=pltpu.VMEM),
        scratch_shapes=[
            vmem((2, HD), BF16),
            vmem((2, HD), BF16),
            vmem((1, 128), I32),
            vmem((2, NSEL, NREQ), I32),
            vmem((2, NFINE, NREQ), I32),
            vmem((SPAN, 2 * HD), BF16),
            vmem((SPAN, 2 * HD), BF16),
            vmem((2 * HD, SPAN), BF16),
            vmem((NZ, 32, HD), BF16),
            vmem((NP, 128, HD), BF16),
            vmem((NP, 128, HD), BF16),
            vmem((NP, NREQ), F32),
            vmem((NY, 32, 256), F32),
            vmem((SPAN, 256), F32),
            vmem((SPAN, 256), BF16),
            vmem((NP, HD, 128), BF16),
            vmem((NP, 1, 128), F32),
            vmem((NP, HD, 128), BF16),
            vmem((NP, 1, 128), F32),
            vmem((NZ, 32, HD), BF16),
            vmem((NZ, 1, 128), F32),
            vmem((NZ, 32, HD), BF16),
            vmem((NZ, 1, 128), F32),
            vmem((NZ, 4, HD), BF16),
            vmem((NZ * 4, HD), F32),
            vmem((NP, NZ * 4, HD), BF16),
            vmem((NX, 8, HD), BF16),
            dma((6,)),
            dma((4,)),
            dma,
            dma,
            dma,
            dma((NY,)),
        ]
        + [dma] * 14
        + [dma((6,))],
        compiler_params=pltpu.CompilerParams(collective_id=0, has_side_effects=True),
    )(
        queries.reshape(32, HD),
        key_cache,
        value_cache,
        summary_keys.reshape(2, HD),
        summary_values.reshape(2, HD),
        owner_map.reshape(1, 128),
        jnp.transpose(super_ids, (1, 2, 0)),
        jnp.transpose(fine_ids, (1, 2, 0)),
    )
    return out.reshape(1, NX * 8, HD)


def solution(mesh):
    in_specs = (
        P("seq", "rep", None),
        P("rep", "seq", None),
        P("rep", "seq", None),
        P("rep", "seq", None),
        P("rep", "seq", None),
        P(),
        P(None, "rep", None),
        P(None, "rep", None),
    )
    return jax.shard_map(
        shards, mesh=mesh, in_specs=in_specs, out_specs=P(("seq", "rep"), None, None), check_vma=False
    )
```

```python
import functools
import math

import jax
import jax.numpy as jnp
from jax import lax
from jax.experimental import pallas as pl
from jax.experimental.pallas import tpu as pltpu
from jax.sharding import PartitionSpec as P

MESH = pl.DeviceIdType.MESH
F32, BF16, I32 = jnp.float32, jnp.bfloat16, jnp.int32
NZ, NP, NY, NX = 16, 8, 4, 4
HD, BLK, SUPER, NSEL, NFINE = 128, 128, 16, 4, 16
NREQ, SPAN = 512, 2048
NEG = -1e30
SCALE2 = HD**-0.5 / math.log(2.0)
Z_ORDER = (8, 7, 9, 6, 10, 5, 11, 4, 12, 3, 13, 2, 14, 1, 15)
PLANE = ((2, 0), (2, 1), (1, 0), (1, 1), (3, 0), (3, 1), (0, 1), (0, 0))


def iota(shape, dim):
    return lax.broadcasted_iota(I32, shape, dim)


def dot(a, b, dims=((1,), (0,))):
    return lax.dot_general(a, b, (dims, ((), ())), preferred_element_type=F32)


def group_rank(hits):
    i = jnp.bitwise_and(iota(hits[0].shape, 1), 3)
    before, total = [], []
    for h in hits:
        b = jnp.zeros_like(h)
        t = h
        for d in (1, 2, 3):
            b = b + jnp.where(i >= d, pltpu.roll(h, d, 1), 0)
            t = t + jnp.where(i + d <= 3, pltpu.roll(h, NREQ - d, 1), 0)
        before.append(b)
        total.append(t + b)
    return before[0], before[1] + total[0]


def kernel(
    q_h, kc_h, vc_h, sk_h, sv_h, om_h, si_h, fi_h, o_ref,
    sk, sv, om, si, fi, kcat, vcat, v_t, qz, qs, rq, rsel, meta, flag, pick, w_s, s_s, p_s,
    os_, ol, ro, rl, pzs, lzs, pz, lz, sz, szf, sf, xs,
    load_sem, kv_sem, q1s, q1r, q2s, q2r, r1s, r1r, l1s, l1r, r2s, r2r, l2s, l2r, szs, szr, sfs, sfr, xss, xsr, loc,
):
    me, rep = lax.axis_index("seq"), lax.axis_index("rep")
    z, p = me // NP, lax.rem(me, NP)
    y, c = p // 2, lax.rem(p, 2)

    def z_peer(d):
        return lax.rem(z + d, NZ)

    def plane_peer(dy, dc):
        return lax.rem(y + dy, NY) * 2 + lax.rem(c + dc, 2)

    plane = PLANE[:-1]

    barrier = pltpu.get_barrier_semaphore()
    for d in Z_ORDER:
        pl.semaphore_signal(barrier, inc=1, device_id=(z_peer(d) * NP + p, rep), device_id_type=MESH)
    for dy, dc in plane:
        pl.semaphore_signal(barrier, inc=1, device_id=(z * NP + plane_peer(dy, dc), rep), device_id_type=MESH)
    for d in range(1, NX):
        pl.semaphore_signal(barrier, inc=1, device_id=(me, lax.rem(rep + d, NX)), device_id_type=MESH)

    def remote(src, dst, ss, rs, seq, x=None):
        return pltpu.make_async_remote_copy(
            src_ref=src, dst_ref=dst, send_sem=ss, recv_sem=rs,
            device_id=(seq, rep if x is None else x), device_id_type=MESH,
        )

    def wait(ref, sem):
        pltpu.make_async_copy(ref, ref, sem).wait()

    loads = [
        pltpu.make_async_copy(a, b, load_sem.at[n])
        for n, (a, b) in enumerate([(q_h, qz.at[z]), (sk_h, sk), (sv_h, sv), (om_h, om), (si_h, si), (fi_h, fi)])
    ]
    kv_loads = [
        pltpu.make_async_copy(a.at[g], b.at[:, pl.ds(g * HD, HD)], kv_sem.at[2 * n + g])
        for n, (a, b) in enumerate([(kc_h, kcat), (vc_h, vcat)])
        for g in (0, 1)
    ]
    for copy in loads + kv_loads:
        copy.start()
    for copy in loads:
        copy.wait()
    sz[z] = jnp.concatenate([sk[...].astype(F32), sv[...].astype(F32)], axis=0).astype(BF16)

    pl.semaphore_wait(barrier, len(Z_ORDER) + len(plane) + NX - 1)

    for d in Z_ORDER:
        remote(qz.at[z], qz.at[z], q1s, q1r, z_peer(d) * NP + p).start()

    omv = om[...]
    siv = [[si[g, j : j + 1, :] for j in range(NSEL)] for g in (0, 1)]
    lane128 = iota((NP, 128), 1)
    sig8 = jnp.sum(jnp.where(omv == z * NP + iota((NP, 128), 0), lane128, 0), axis=1, keepdims=True)
    hits = []
    for g in (0, 1):
        h = siv[g][0] == sig8
        for j in range(1, NSEL):
            h = jnp.logical_or(h, siv[g][j] == sig8)
        hits.append(jnp.where(h, 1, 0))
    ranks = group_rank(hits)
    row, lane = iota((NREQ, NREQ), 0), iota((NREQ, NREQ), 1)
    source = (lane >> 5) * 32 + p * 4 + ((lane >> 3) & 3)
    picked = jnp.zeros((NP, NREQ), F32)
    for g in (0, 1):
        spread = jnp.where(row == jnp.where(((lane >> 2) & 1) == g, source, -1), 1.0, 0.0).astype(BF16)
        code = jnp.where(hits[g] > 0, ranks[g] + 1, 0).astype(F32).astype(BF16)
        picked = picked + dot(code, spread)
    rsel[...] = picked

    sig1 = jnp.sum(jnp.where(omv == me, lane128[0:1], 0), axis=1, keepdims=True)
    own_hits, own_bits = [], []
    for g in (0, 1):
        h, jsel = jnp.zeros((1, NREQ), I32), jnp.zeros((1, NREQ), I32)
        for j in range(NSEL):
            same = siv[g][j] == sig1
            h = jnp.where(same, 1, h)
            jsel = jnp.where(same, j, jsel)
        target = jsel * SUPER + iota((SUPER, NREQ), 0)
        bits = fi[g, 0:1, :] == target
        for k in range(1, NFINE):
            bits = jnp.logical_or(bits, fi[g, k : k + 1, :] == target)
        own_hits.append(jnp.broadcast_to(h, (8, NREQ)))
        own_bits.append(jnp.where(bits, 1.0, 0.0))
    own_ranks = group_rank(own_hits)
    sub8 = iota((8, NREQ), 0)
    stacked = []
    for slot in (0, 1):
        use = [jnp.where(jnp.logical_and(own_hits[g] > 0, own_ranks[g] == slot), 1.0, 0.0) for g in (0, 1)]
        wanted = own_bits[0] * use[0][0:1] + own_bits[1] * use[1][0:1]
        flags = jnp.where(sub8 == 0, use[0], jnp.where(sub8 == 1, use[1], 0.0))
        stacked.append(jnp.concatenate([wanted, flags, jnp.zeros((8, NREQ), F32)], axis=0).astype(BF16))
    for chunk in range(NY):
        row, col = iota((NREQ, 256), 0), iota((NREQ, 256), 1)
        sender = ((col >> 3) & 15) * NP + chunk * 2 + (col >> 7)
        acc = jnp.zeros((32, 256), F32)
        for slot in (0, 1):
            at = jnp.where(((col >> 2) & 1) == slot, sender, -1)
            acc = acc + dot(stacked[slot], jnp.where((row >> 2) == at, 1.0, 0.0).astype(BF16))
        meta[chunk] = acc
        flag[chunk] = jnp.transpose(acc[16:24], (1, 0))

    brow, blane = iota((32, 128), 0), iota((32, 128), 1)
    base = jnp.where(
        jnp.logical_and((brow >> 3) == (blane >> 5), (brow & 3) == (blane & 3)), ((brow >> 2) & 1) + 1, -1
    ).astype(F32)
    pick[...] = jnp.zeros_like(pick)
    w_s[...] = jnp.zeros_like(w_s)
    for n, (dy, dc) in enumerate(PLANE):
        code = rsel[pl.ds(plane_peer(dy, dc), 1), :]
        for b in range(4):
            same = base == code[:, b * 128 : (b + 1) * 128]
            pick[n * 128 + b * 32 : n * 128 + (b + 1) * 32, b * 128 : (b + 1) * 128] = jnp.where(
                same, 1.0, 0.0
            ).astype(BF16)
    for copy in kv_loads:
        copy.wait()
    v_t[...] = jnp.transpose(vcat[...], (1, 0))

    wait(qz.at[pl.ds(0, NZ - 1)], q1r)
    every = qz[...].reshape(NREQ, HD)
    for half in (0, 1):
        rows = dot(pick[half * 512 : (half + 1) * 512, :], every).astype(BF16)
        qs[half * 4 : half * 4 + 4] = rows.reshape(4, 128, HD)
        for n in range(half * 4, half * 4 + 4):
            dy, dc = PLANE[n]
            if dy or dc:
                remote(qs.at[n], rq.at[p], q2s, q2r.at[dy], z * NP + plane_peer(dy, dc)).start()
            else:
                pltpu.make_async_copy(qs.at[n], rq.at[p], loc.at[0]).start()
    for d in Z_ORDER:
        remote(sz.at[z], sz.at[z], szs, szr, z_peer(d) * NP + p).start()
    wait(qs.at[0], loc.at[0])

    def chunk_step(turn, carry):
        k = jnp.where(turn == 2, 3, jnp.where(turn == 3, 2, turn))

        @pl.when(k == 0)
        def _():
            wait(rq.at[0], q2r.at[0])

        @pl.when(k > 0)
        def _():
            wait(rq.at[pl.ds(0, 2)], q2r.at[k])

        yy = lax.rem(y + NY - k, NY)
        m_all = meta[yy]
        flags = flag[yy].astype(BF16)
        rows = rq[pl.ds(yy * 2, 2)].reshape(256, HD)
        split = jnp.concatenate([rows * flags[:, 0:1], rows * flags[:, 1:2]], axis=1)
        s_s[...] = dot(kcat[...], split, ((1,), (1,)))
        bias = jnp.where(m_all[0:16] > 0.5, 0.0, NEG)
        peak = jnp.full((1, 256), -3e38, F32)
        for b in range(SUPER):
            top = jnp.max(s_s[b * BLK : (b + 1) * BLK, :], axis=0, keepdims=True)
            peak = jnp.maximum(peak, top + bias[b : b + 1])
        total = jnp.zeros((1, 256), F32)
        for b in range(SUPER):
            w = jnp.exp2((s_s[b * BLK : (b + 1) * BLK, :] + (bias[b : b + 1] - peak)) * SCALE2)
            total = total + jnp.sum(w, axis=0, keepdims=True)
            p_s[b * BLK : (b + 1) * BLK, :] = w.astype(BF16)
        out = dot(v_t[...], p_s[...])
        out = jnp.where(m_all[17:18] > 0.5, out[HD : 2 * HD], out[0:HD]) * (1.0 / total)
        log_sum = peak * SCALE2 + jnp.log2(total)
        for n in (0, 1):
            os_[yy * 2 + n] = out[:, n * 128 : (n + 1) * 128].astype(BF16)
            ol[yy * 2 + n] = log_sum[:, n * 128 : (n + 1) * 128]

        mine, other = yy * 2 + c, yy * 2 + 1 - c

        @pl.when(k == 0)
        def _():
            pltpu.make_async_copy(os_.at[mine], ro.at[mine], loc.at[1]).start()
            pltpu.make_async_copy(ol.at[mine], rl.at[mine], loc.at[2]).start()

        @pl.when(k > 0)
        def _():
            remote(os_.at[mine], ro.at[p], r1s, r1r, z * NP + mine).start()
            remote(ol.at[mine], rl.at[p], l1s, l1r, z * NP + mine).start()

        remote(os_.at[other], ro.at[p], r1s, r1r, z * NP + other).start()
        remote(ol.at[other], rl.at[p], l1s, l1r, z * NP + other).start()
        return carry

    lax.fori_loop(0, NY, chunk_step, 0)

    wait(sz.at[pl.ds(0, NZ - 1)], szr)
    for n in range(NZ):
        szf[n * 4 : n * 4 + 4, :] = sz[n].astype(F32)
    sf[p] = szf[...].astype(BF16)
    for dy, dc in plane:
        remote(sf.at[p], sf.at[p], sfs, sfr, z * NP + plane_peer(dy, dc)).start()

    wait(os_.at[0], loc.at[1])
    wait(ol.at[0], loc.at[2])
    wait(ro.at[pl.ds(0, NP - 1)], r1r)
    wait(rl.at[pl.ds(0, NP - 1)], l1r)
    l_cols = jnp.transpose(rl[...].reshape(NP, 128), (1, 0))
    same = [[base == rsel[n : n + 1, b * 128 : (b + 1) * 128] for b in range(4)] for n in range(NP)]
    peaks, totals = [], []
    for b in range(4):
        peak = jnp.full((32, 128), NEG, F32)
        for n in range(NP):
            peak = jnp.maximum(peak, jnp.where(same[n][b], l_cols[b * 32 : (b + 1) * 32, n : n + 1], NEG))
        peak = jnp.max(peak, axis=0, keepdims=True)
        total = jnp.zeros((32, 128), F32)
        for n in range(NP):
            w = jnp.where(same[n][b], jnp.exp2(l_cols[b * 32 : (b + 1) * 32, n : n + 1] - peak), 0.0)
            total = total + w
            w_s[n * 128 + b * 32 : n * 128 + (b + 1) * 32, b * 128 : (b + 1) * 128] = w.astype(BF16)
        peaks.append(peak)
        totals.append(jnp.sum(total, axis=0, keepdims=True))
    peak, total = jnp.concatenate(peaks, axis=1), jnp.concatenate(totals, axis=1)
    merged = jnp.zeros((HD, NREQ), F32)
    for n in range(0, NP, 2):
        pair = jnp.concatenate([ro[n], ro[n + 1]], axis=1)
        merged = merged + dot(pair, w_s[n * 128 : (n + 2) * 128, :])
    some = total > 0.0
    merged = merged * jnp.where(some, 1.0 / jnp.where(some, total, 1.0), 0.0)
    log_sum = jnp.where(some, peak + jnp.log2(jnp.where(some, total, 1.0)), NEG)
    pzs[...] = jnp.transpose(merged, (1, 0)).astype(BF16).reshape(NZ, 32, HD)
    for n in range(NZ):
        part = log_sum[:, (n // 4) * 128 : (n // 4) * 128 + 128]
        lzs[n] = pltpu.roll(part, 128 - 32 * (n % 4), 1) if n % 4 else part
    keep = [
        pltpu.make_async_copy(pzs.at[z], pz.at[z], loc.at[3]),
        pltpu.make_async_copy(lzs.at[z], lz.at[z], loc.at[4]),
    ]
    for copy in keep:
        copy.start()
    for d in Z_ORDER:
        zz = z_peer(d)
        remote(pzs.at[zz], pz.at[z], r2s, r2r, zz * NP + p).start()
        remote(lzs.at[zz], lz.at[z], l2s, l2r, zz * NP + p).start()
    for copy in keep:
        copy.wait()

    wait(sf.at[pl.ds(0, NP - 1)], sfr)
    every_summary = sf[...].reshape(NREQ, HD)
    erow, elane = iota((128, 128), 0), iota((128, 128), 1)
    om_col = jnp.sum(jnp.where(erow == elane, omv, 0), axis=1, keepdims=True)
    tok = iota((1, NREQ), 1)
    tok_slot = ((tok >> 2) & 15) * NP + (tok >> 6)
    tok_super = jnp.sum(jnp.where(om_col == tok_slot, iota((128, NREQ), 0), 0), axis=0, keepdims=True)
    r_head, r_tok = iota((32, NREQ), 0), iota((32, NREQ), 1)
    r_group = (r_head >> 2) & 1
    kept = (r_tok & 3) == r_group
    for j in range(NSEL):
        ids = jnp.where(r_group == 0, siv[0][j], siv[1][j])
        own = jnp.sum(jnp.where(r_tok == me * 4 + (r_head >> 3), ids, 0), axis=1, keepdims=True)
        kept = jnp.logical_and(kept, tok_super != own)
    c_score = dot(qz[z], every_summary, ((1,), (1,))) * SCALE2 + 4.0
    c_score = jnp.where(kept, c_score, NEG)
    c_peak = jnp.max(c_score, axis=1, keepdims=True)
    c_w = jnp.where(kept, jnp.exp2(c_score - c_peak), 0.0)
    c_sum = jnp.sum(c_w, axis=1, keepdims=True)
    c_out = dot(pltpu.roll(c_w, 2, 1).astype(BF16), every_summary)

    wait(pz.at[pl.ds(0, NZ - 1)], r2r)
    wait(lz.at[pl.ds(0, NZ - 1)], l2r)

    lse = jnp.transpose(lz[...].reshape(NZ, 128), (1, 0))[0:32]
    c_lse = c_peak + jnp.log2(c_sum)
    top = jnp.maximum(jnp.max(lse, axis=1, keepdims=True), c_lse)
    w = jnp.exp2(lse - top)
    c_scale = jnp.exp2(c_peak - top)
    total = jnp.sum(w, axis=1, keepdims=True) + c_scale * c_sum
    result = c_out * c_scale
    for n in range(NZ):
        result = result + pz[n].astype(F32) * w[:, n : n + 1]
    xs[...] = (result / total).astype(BF16).reshape(NX, 8, HD)
    keep = pltpu.make_async_copy(xs.at[rep], o_ref.at[rep], loc.at[5])
    keep.start()
    for d in range(1, NX):
        x = lax.rem(rep + d, NX)
        remote(xs.at[x], o_ref.at[rep], xss, xsr, me, x).start()

    wait(qz.at[pl.ds(0, NZ - 1)], q1s)
    wait(sz.at[pl.ds(0, NZ - 1)], szs)
    wait(qs.at[pl.ds(0, NP - 1)], q2s)
    wait(sf.at[pl.ds(0, NP - 1)], sfs)
    wait(os_.at[pl.ds(0, NP - 1)], r1s)
    wait(ol.at[pl.ds(0, NP - 1)], l1s)
    wait(pzs.at[pl.ds(0, NZ - 1)], r2s)
    wait(lzs.at[pl.ds(0, NZ - 1)], l2s)
    keep.wait()
    wait(xs.at[pl.ds(0, NX - 1)], xss)
    wait(o_ref.at[pl.ds(0, NX - 1)], xsr)


def shards(queries, key_cache, value_cache, summary_keys, summary_values, owner_map, super_ids, fine_ids):
    vmem, dma = pltpu.VMEM, pltpu.SemaphoreType.DMA
    out = pl.pallas_call(
        kernel,
        out_shape=jax.ShapeDtypeStruct((NX, 8, HD), BF16),
        in_specs=[pl.BlockSpec(memory_space=pltpu.HBM)] * 8,
        out_specs=pl.BlockSpec(memory_space=pltpu.VMEM),
        scratch_shapes=[
            vmem((2, HD), BF16),
            vmem((2, HD), BF16),
            vmem((1, 128), I32),
            vmem((2, NSEL, NREQ), I32),
            vmem((2, NFINE, NREQ), I32),
            vmem((SPAN, 2 * HD), BF16),
            vmem((SPAN, 2 * HD), BF16),
            vmem((2 * HD, SPAN), BF16),
            vmem((NZ, 32, HD), BF16),
            vmem((NP, 128, HD), BF16),
            vmem((NP, 128, HD), BF16),
            vmem((NP, NREQ), F32),
            vmem((NY, 32, 256), F32),
            vmem((NY, 256, 8), F32),
            vmem((NP * 128, NREQ), BF16),
            vmem((NP * 128, NREQ), BF16),
            vmem((SPAN, 256), F32),
            vmem((SPAN, 256), BF16),
            vmem((NP, HD, 128), BF16),
            vmem((NP, 1, 128), F32),
            vmem((NP, HD, 128), BF16),
            vmem((NP, 1, 128), F32),
            vmem((NZ, 32, HD), BF16),
            vmem((NZ, 1, 128), F32),
            vmem((NZ, 32, HD), BF16),
            vmem((NZ, 1, 128), F32),
            vmem((NZ, 4, HD), BF16),
            vmem((NZ * 4, HD), F32),
            vmem((NP, NZ * 4, HD), BF16),
            vmem((NX, 8, HD), BF16),
            dma((6,)),
            dma((4,)),
            dma,
            dma,
            dma,
            dma((NY,)),
        ]
        + [dma] * 14
        + [dma((6,))],
        compiler_params=pltpu.CompilerParams(collective_id=0, has_side_effects=True),
    )(
        queries.reshape(32, HD),
        key_cache,
        value_cache,
        summary_keys.reshape(2, HD),
        summary_values.reshape(2, HD),
        owner_map.reshape(1, 128),
        jnp.transpose(super_ids, (1, 2, 0)),
        jnp.transpose(fine_ids, (1, 2, 0)),
    )
    return out.reshape(1, NX * 8, HD)


def solution(mesh):
    in_specs = (
        P("seq", "rep", None),
        P("rep", "seq", None),
        P("rep", "seq", None),
        P("rep", "seq", None),
        P("rep", "seq", None),
        P(),
        P(None, "rep", None),
        P(None, "rep", None),
    )
    return jax.shard_map(
        shards, mesh=mesh, in_specs=in_specs, out_specs=P(("seq", "rep"), None, None), check_vma=False
    )
```

```python
import functools
import math

import jax
import jax.numpy as jnp
from jax import lax
from jax.experimental import pallas as pl
from jax.experimental.pallas import tpu as pltpu
from jax.sharding import PartitionSpec as P

MESH = pl.DeviceIdType.MESH
F32, BF16, I32 = jnp.float32, jnp.bfloat16, jnp.int32
NZ, NP, NY, NX = 16, 8, 4, 4
HD, BLK, SUPER, NSEL, NFINE = 128, 128, 16, 4, 16
NREQ, SPAN = 512, 2048
NEG = -1e30
SCALE2 = HD**-0.5 / math.log(2.0)
Z_ORDER = (8, 7, 9, 6, 10, 5, 11, 4, 12, 3, 13, 2, 14, 1, 15)
PARTS = 4
PLANE = ((2, 0), (2, 1), (1, 0), (1, 1), (3, 0), (3, 1), (0, 1), (0, 0))


def iota(shape, dim):
    return lax.broadcasted_iota(I32, shape, dim)


def dot(a, b, dims=((1,), (0,))):
    return lax.dot_general(a, b, (dims, ((), ())), preferred_element_type=F32)


def group_rank(hits):
    i = jnp.bitwise_and(iota(hits[0].shape, 1), 3)
    before, total = [], []
    for h in hits:
        b = jnp.zeros_like(h)
        t = h
        for d in (1, 2, 3):
            b = b + jnp.where(i >= d, pltpu.roll(h, d, 1), 0)
            t = t + jnp.where(i + d <= 3, pltpu.roll(h, NREQ - d, 1), 0)
        before.append(b)
        total.append(t + b)
    return before[0], before[1] + total[0]


def kernel(
    q_h, kc_h, vc_h, sk_h, sv_h, om_h, si_h, fi_h, o_ref,
    sk, sv, om, si, fi, kcat, vcat, v_t, qz, qs, rq, rsel, meta, flag, pick, w_s,
    os_, ol, ro, rl, pzs, lzs, pz, lz, sz, szf, sf, xs,
    load_sem, kv_sem, q1s, q1r, q2s, q2r, r1s, r1r, l1s, l1r, r2s, r2r, l2s, l2r, szs, szr, sfs, sfr, xss, xsr, loc,
):
    me, rep = lax.axis_index("seq"), lax.axis_index("rep")
    z, p = me // NP, lax.rem(me, NP)
    y, c = p // 2, lax.rem(p, 2)

    def z_peer(d):
        return lax.rem(z + d, NZ)

    def plane_peer(dy, dc):
        return lax.rem(y + dy, NY) * 2 + lax.rem(c + dc, 2)

    plane = PLANE[:-1]

    barrier = pltpu.get_barrier_semaphore()
    for d in Z_ORDER:
        pl.semaphore_signal(barrier, inc=1, device_id=(z_peer(d) * NP + p, rep), device_id_type=MESH)
    for dy, dc in plane:
        pl.semaphore_signal(barrier, inc=1, device_id=(z * NP + plane_peer(dy, dc), rep), device_id_type=MESH)
    for d in range(1, NX):
        pl.semaphore_signal(barrier, inc=1, device_id=(me, lax.rem(rep + d, NX)), device_id_type=MESH)

    def remote(src, dst, ss, rs, seq, x=None):
        return pltpu.make_async_remote_copy(
            src_ref=src, dst_ref=dst, send_sem=ss, recv_sem=rs,
            device_id=(seq, rep if x is None else x), device_id_type=MESH,
        )

    def wait(ref, sem):
        pltpu.make_async_copy(ref, ref, sem).wait()

    loads = [
        pltpu.make_async_copy(a, b, load_sem.at[n])
        for n, (a, b) in enumerate([(q_h, qz.at[z]), (sk_h, sk), (sv_h, sv), (om_h, om), (si_h, si), (fi_h, fi)])
    ]
    kv_loads = [
        pltpu.make_async_copy(a.at[g], b.at[:, pl.ds(g * HD, HD)], kv_sem.at[2 * n + g])
        for n, (a, b) in enumerate([(kc_h, kcat), (vc_h, vcat)])
        for g in (0, 1)
    ]
    for copy in loads + kv_loads:
        copy.start()
    for copy in loads:
        copy.wait()
    sz[z] = jnp.concatenate([sk[...].astype(F32), sv[...].astype(F32)], axis=0).astype(BF16)

    pl.semaphore_wait(barrier, len(Z_ORDER) + len(plane) + NX - 1)

    for d in Z_ORDER:
        remote(qz.at[z], qz.at[z], q1s, q1r, z_peer(d) * NP + p).start()

    omv = om[...]
    siv = [[si[g, j : j + 1, :] for j in range(NSEL)] for g in (0, 1)]
    lane128 = iota((NP, 128), 1)
    sig8 = jnp.sum(jnp.where(omv == z * NP + iota((NP, 128), 0), lane128, 0), axis=1, keepdims=True)
    hits = []
    for g in (0, 1):
        h = siv[g][0] == sig8
        for j in range(1, NSEL):
            h = jnp.logical_or(h, siv[g][j] == sig8)
        hits.append(jnp.where(h, 1, 0))
    ranks = group_rank(hits)
    row, lane = iota((NREQ, NREQ), 0), iota((NREQ, NREQ), 1)
    source = (lane >> 5) * 32 + p * 4 + ((lane >> 3) & 3)
    picked = jnp.zeros((NP, NREQ), F32)
    for g in (0, 1):
        spread = jnp.where(row == jnp.where(((lane >> 2) & 1) == g, source, -1), 1.0, 0.0).astype(BF16)
        code = jnp.where(hits[g] > 0, ranks[g] + 1, 0).astype(F32).astype(BF16)
        picked = picked + dot(code, spread)
    rsel[...] = picked

    sig1 = jnp.sum(jnp.where(omv == me, lane128[0:1], 0), axis=1, keepdims=True)
    own_hits, own_bits = [], []
    for g in (0, 1):
        h, jsel = jnp.zeros((1, NREQ), I32), jnp.zeros((1, NREQ), I32)
        for j in range(NSEL):
            same = siv[g][j] == sig1
            h = jnp.where(same, 1, h)
            jsel = jnp.where(same, j, jsel)
        target = jsel * SUPER + iota((SUPER, NREQ), 0)
        bits = fi[g, 0:1, :] == target
        for k in range(1, NFINE):
            bits = jnp.logical_or(bits, fi[g, k : k + 1, :] == target)
        own_hits.append(jnp.broadcast_to(h, (8, NREQ)))
        own_bits.append(jnp.where(bits, 1.0, 0.0))
    own_ranks = group_rank(own_hits)
    sub8 = iota((8, NREQ), 0)
    stacked = []
    for slot in (0, 1):
        use = [jnp.where(jnp.logical_and(own_hits[g] > 0, own_ranks[g] == slot), 1.0, 0.0) for g in (0, 1)]
        wanted = own_bits[0] * use[0][0:1] + own_bits[1] * use[1][0:1]
        flags = jnp.where(sub8 == 0, use[0], jnp.where(sub8 == 1, use[1], 0.0))
        stacked.append(jnp.concatenate([wanted, flags, jnp.zeros((8, NREQ), F32)], axis=0).astype(BF16))
    for chunk in range(NY):
        row, col = iota((NREQ, 256), 0), iota((NREQ, 256), 1)
        sender = ((col >> 3) & 15) * NP + chunk * 2 + (col >> 7)
        acc = jnp.zeros((32, 256), F32)
        for slot in (0, 1):
            at = jnp.where(((col >> 2) & 1) == slot, sender, -1)
            acc = acc + dot(stacked[slot], jnp.where((row >> 2) == at, 1.0, 0.0).astype(BF16))
        meta[chunk] = acc
        flag[chunk] = jnp.transpose(acc[16:24], (1, 0))

    brow, blane = iota((32, 128), 0), iota((32, 128), 1)
    base = jnp.where(
        jnp.logical_and((brow >> 3) == (blane >> 5), (brow & 3) == (blane & 3)), ((brow >> 2) & 1) + 1, -1
    ).astype(F32)
    pick[...] = jnp.zeros_like(pick)
    w_s[...] = jnp.zeros_like(w_s)
    for n, (dy, dc) in enumerate(PLANE):
        code = rsel[pl.ds(plane_peer(dy, dc), 1), :]
        for b in range(4):
            same = base == code[:, b * 128 : (b + 1) * 128]
            pick[n * 128 + b * 32 : n * 128 + (b + 1) * 32, b * 128 : (b + 1) * 128] = jnp.where(
                same, 1.0, 0.0
            ).astype(BF16)
    for copy in kv_loads:
        copy.wait()
    v_t[...] = jnp.transpose(vcat[...], (1, 0))

    wait(qz.at[pl.ds(0, NZ - 1)], q1r)
    every = qz[...].reshape(NREQ, HD)
    for half in (0, 1):
        rows = dot(pick[half * 512 : (half + 1) * 512, :], every).astype(BF16)
        qs[half * 4 : half * 4 + 4] = rows.reshape(4, 128, HD)
        for n in range(half * 4, half * 4 + 4):
            dy, dc = PLANE[n]
            if dy or dc:
                remote(qs.at[n], rq.at[p], q2s, q2r.at[dy], z * NP + plane_peer(dy, dc)).start()
            else:
                pltpu.make_async_copy(qs.at[n], rq.at[p], loc.at[0]).start()
    for d in Z_ORDER:
        remote(sz.at[z], sz.at[z], szs, szr, z_peer(d) * NP + p).start()
    wait(qs.at[0], loc.at[0])

    def chunk_step(turn, carry):
        k = jnp.where(turn == 2, 3, jnp.where(turn == 3, 2, turn))

        @pl.when(k == 0)
        def _():
            wait(rq.at[0], q2r.at[0])

        @pl.when(k > 0)
        def _():
            wait(rq.at[pl.ds(0, 2)], q2r.at[k])

        yy = lax.rem(y + NY - k, NY)
        m_all = meta[yy]
        flags = flag[yy].astype(BF16)
        rows = rq[pl.ds(yy * 2, 2)].reshape(256, HD)
        split = jnp.concatenate([rows * flags[:, 0:1], rows * flags[:, 1:2]], axis=1)
        bias = jnp.where(m_all[0:16] > 0.5, 0.0, NEG)
        span, per = SPAN // PARTS, SUPER // PARTS
        outs, peaks, totals = [], [], []
        for t in range(PARTS):
            s = dot(kcat[t * span : (t + 1) * span, :], split, ((1,), (1,)))
            top = jnp.full((1, 256), -3e38, F32)
            for b in range(per):
                one = jnp.max(s[b * BLK : (b + 1) * BLK], axis=0, keepdims=True)
                top = jnp.maximum(top, one + bias[t * per + b : t * per + b + 1])
            part, ws = jnp.zeros((1, 256), F32), []
            for b in range(per):
                w = jnp.exp2((s[b * BLK : (b + 1) * BLK] + (bias[t * per + b : t * per + b + 1] - top)) * SCALE2)
                part = part + jnp.sum(w, axis=0, keepdims=True)
                ws.append(w.astype(BF16))
            outs.append(dot(v_t[:, t * span : (t + 1) * span], jnp.concatenate(ws, axis=0)))
            peaks.append(top)
            totals.append(part)
        peak = functools.reduce(jnp.maximum, peaks)
        factors = [jnp.exp2((top - peak) * SCALE2) for top in peaks]
        total = sum(f * part for f, part in zip(factors, totals))
        out = sum(f * o for f, o in zip(factors, outs))
        out = jnp.where(m_all[17:18] > 0.5, out[HD : 2 * HD], out[0:HD]) * (1.0 / total)
        log_sum = peak * SCALE2 + jnp.log2(total)
        for n in (0, 1):
            os_[yy * 2 + n] = out[:, n * 128 : (n + 1) * 128].astype(BF16)
            ol[yy * 2 + n] = log_sum[:, n * 128 : (n + 1) * 128]

        mine, other = yy * 2 + c, yy * 2 + 1 - c

        @pl.when(k == 0)
        def _():
            pltpu.make_async_copy(os_.at[mine], ro.at[mine], loc.at[1]).start()
            pltpu.make_async_copy(ol.at[mine], rl.at[mine], loc.at[2]).start()

        @pl.when(k > 0)
        def _():
            remote(os_.at[mine], ro.at[p], r1s, r1r, z * NP + mine).start()
            remote(ol.at[mine], rl.at[p], l1s, l1r, z * NP + mine).start()

        remote(os_.at[other], ro.at[p], r1s, r1r, z * NP + other).start()
        remote(ol.at[other], rl.at[p], l1s, l1r, z * NP + other).start()
        return carry

    lax.fori_loop(0, NY, chunk_step, 0)

    wait(sz.at[pl.ds(0, NZ - 1)], szr)
    for n in range(NZ):
        szf[n * 4 : n * 4 + 4, :] = sz[n].astype(F32)
    sf[p] = szf[...].astype(BF16)
    for dy, dc in plane:
        remote(sf.at[p], sf.at[p], sfs, sfr, z * NP + plane_peer(dy, dc)).start()

    wait(os_.at[0], loc.at[1])
    wait(ol.at[0], loc.at[2])
    wait(ro.at[pl.ds(0, NP - 1)], r1r)
    wait(rl.at[pl.ds(0, NP - 1)], l1r)
    l_cols = jnp.transpose(rl[...].reshape(NP, 128), (1, 0))
    same = [[base == rsel[n : n + 1, b * 128 : (b + 1) * 128] for b in range(4)] for n in range(NP)]
    peaks, totals = [], []
    for b in range(4):
        peak = jnp.full((32, 128), NEG, F32)
        for n in range(NP):
            peak = jnp.maximum(peak, jnp.where(same[n][b], l_cols[b * 32 : (b + 1) * 32, n : n + 1], NEG))
        peak = jnp.max(peak, axis=0, keepdims=True)
        total = jnp.zeros((32, 128), F32)
        for n in range(NP):
            w = jnp.where(same[n][b], jnp.exp2(l_cols[b * 32 : (b + 1) * 32, n : n + 1] - peak), 0.0)
            total = total + w
            w_s[n * 128 + b * 32 : n * 128 + (b + 1) * 32, b * 128 : (b + 1) * 128] = w.astype(BF16)
        peaks.append(peak)
        totals.append(jnp.sum(total, axis=0, keepdims=True))
    peak, total = jnp.concatenate(peaks, axis=1), jnp.concatenate(totals, axis=1)
    merged = jnp.zeros((HD, NREQ), F32)
    for n in range(0, NP, 2):
        pair = jnp.concatenate([ro[n], ro[n + 1]], axis=1)
        merged = merged + dot(pair, w_s[n * 128 : (n + 2) * 128, :])
    some = total > 0.0
    merged = merged * jnp.where(some, 1.0 / jnp.where(some, total, 1.0), 0.0)
    log_sum = jnp.where(some, peak + jnp.log2(jnp.where(some, total, 1.0)), NEG)
    pzs[...] = jnp.transpose(merged, (1, 0)).astype(BF16).reshape(NZ, 32, HD)
    for n in range(NZ):
        part = log_sum[:, (n // 4) * 128 : (n // 4) * 128 + 128]
        lzs[n] = pltpu.roll(part, 128 - 32 * (n % 4), 1) if n % 4 else part
    keep = [
        pltpu.make_async_copy(pzs.at[z], pz.at[z], loc.at[3]),
        pltpu.make_async_copy(lzs.at[z], lz.at[z], loc.at[4]),
    ]
    for copy in keep:
        copy.start()
    for d in Z_ORDER:
        zz = z_peer(d)
        remote(pzs.at[zz], pz.at[z], r2s, r2r, zz * NP + p).start()
        remote(lzs.at[zz], lz.at[z], l2s, l2r, zz * NP + p).start()
    for copy in keep:
        copy.wait()

    wait(sf.at[pl.ds(0, NP - 1)], sfr)
    every_summary = sf[...].reshape(NREQ, HD)
    erow, elane = iota((128, 128), 0), iota((128, 128), 1)
    om_col = jnp.sum(jnp.where(erow == elane, omv, 0), axis=1, keepdims=True)
    tok = iota((1, NREQ), 1)
    tok_slot = ((tok >> 2) & 15) * NP + (tok >> 6)
    tok_super = jnp.sum(jnp.where(om_col == tok_slot, iota((128, NREQ), 0), 0), axis=0, keepdims=True)
    r_head, r_tok = iota((32, NREQ), 0), iota((32, NREQ), 1)
    r_group = (r_head >> 2) & 1
    kept = (r_tok & 3) == r_group
    for j in range(NSEL):
        ids = jnp.where(r_group == 0, siv[0][j], siv[1][j])
        own = jnp.sum(jnp.where(r_tok == me * 4 + (r_head >> 3), ids, 0), axis=1, keepdims=True)
        kept = jnp.logical_and(kept, tok_super != own)
    c_score = dot(qz[z], every_summary, ((1,), (1,))) * SCALE2 + 4.0
    c_score = jnp.where(kept, c_score, NEG)
    c_peak = jnp.max(c_score, axis=1, keepdims=True)
    c_w = jnp.where(kept, jnp.exp2(c_score - c_peak), 0.0)
    c_sum = jnp.sum(c_w, axis=1, keepdims=True)
    c_out = dot(pltpu.roll(c_w, 2, 1).astype(BF16), every_summary)

    wait(pz.at[pl.ds(0, NZ - 1)], r2r)
    wait(lz.at[pl.ds(0, NZ - 1)], l2r)

    lse = jnp.transpose(lz[...].reshape(NZ, 128), (1, 0))[0:32]
    c_lse = c_peak + jnp.log2(c_sum)
    top = jnp.maximum(jnp.max(lse, axis=1, keepdims=True), c_lse)
    w = jnp.exp2(lse - top)
    c_scale = jnp.exp2(c_peak - top)
    total = jnp.sum(w, axis=1, keepdims=True) + c_scale * c_sum
    result = c_out * c_scale
    for n in range(NZ):
        result = result + pz[n].astype(F32) * w[:, n : n + 1]
    xs[...] = (result / total).astype(BF16).reshape(NX, 8, HD)
    keep = pltpu.make_async_copy(xs.at[rep], o_ref.at[rep], loc.at[5])
    keep.start()
    for d in range(1, NX):
        x = lax.rem(rep + d, NX)
        remote(xs.at[x], o_ref.at[rep], xss, xsr, me, x).start()

    wait(qz.at[pl.ds(0, NZ - 1)], q1s)
    wait(sz.at[pl.ds(0, NZ - 1)], szs)
    wait(qs.at[pl.ds(0, NP - 1)], q2s)
    wait(sf.at[pl.ds(0, NP - 1)], sfs)
    wait(os_.at[pl.ds(0, NP - 1)], r1s)
    wait(ol.at[pl.ds(0, NP - 1)], l1s)
    wait(pzs.at[pl.ds(0, NZ - 1)], r2s)
    wait(lzs.at[pl.ds(0, NZ - 1)], l2s)
    keep.wait()
    wait(xs.at[pl.ds(0, NX - 1)], xss)
    wait(o_ref.at[pl.ds(0, NX - 1)], xsr)


def shards(queries, key_cache, value_cache, summary_keys, summary_values, owner_map, super_ids, fine_ids):
    vmem, dma = pltpu.VMEM, pltpu.SemaphoreType.DMA
    out = pl.pallas_call(
        kernel,
        out_shape=jax.ShapeDtypeStruct((NX, 8, HD), BF16),
        in_specs=[pl.BlockSpec(memory_space=pltpu.HBM)] * 8,
        out_specs=pl.BlockSpec(memory_space=pltpu.HBM),
        scratch_shapes=[
            vmem((2, HD), BF16),
            vmem((2, HD), BF16),
            vmem((1, 128), I32),
            vmem((2, NSEL, NREQ), I32),
            vmem((2, NFINE, NREQ), I32),
            vmem((SPAN, 2 * HD), BF16),
            vmem((SPAN, 2 * HD), BF16),
            vmem((2 * HD, SPAN), BF16),
            vmem((NZ, 32, HD), BF16),
            vmem((NP, 128, HD), BF16),
            vmem((NP, 128, HD), BF16),
            vmem((NP, NREQ), F32),
            vmem((NY, 32, 256), F32),
            vmem((NY, 256, 8), F32),
            vmem((NP * 128, NREQ), BF16),
            vmem((NP * 128, NREQ), BF16),
            vmem((NP, HD, 128), BF16),
            vmem((NP, 1, 128), F32),
            vmem((NP, HD, 128), BF16),
            vmem((NP, 1, 128), F32),
            vmem((NZ, 32, HD), BF16),
            vmem((NZ, 1, 128), F32),
            vmem((NZ, 32, HD), BF16),
            vmem((NZ, 1, 128), F32),
            vmem((NZ, 4, HD), BF16),
            vmem((NZ * 4, HD), F32),
            vmem((NP, NZ * 4, HD), BF16),
            vmem((NX, 8, HD), BF16),
            dma((6,)),
            dma((4,)),
            dma,
            dma,
            dma,
            dma((NY,)),
        ]
        + [dma] * 14
        + [dma((6,))],
        compiler_params=pltpu.CompilerParams(collective_id=0, has_side_effects=True),
    )(
        queries.reshape(32, HD),
        key_cache,
        value_cache,
        summary_keys.reshape(2, HD),
        summary_values.reshape(2, HD),
        owner_map.reshape(1, 128),
        jnp.transpose(super_ids, (1, 2, 0)),
        jnp.transpose(fine_ids, (1, 2, 0)),
    )
    return out.reshape(1, NX * 8, HD)


def solution(mesh):
    in_specs = (
        P("seq", "rep", None),
        P("rep", "seq", None),
        P("rep", "seq", None),
        P("rep", "seq", None),
        P("rep", "seq", None),
        P(),
        P(None, "rep", None),
        P(None, "rep", None),
    )
    return jax.shard_map(
        shards, mesh=mesh, in_specs=in_specs, out_specs=P(("seq", "rep"), None, None), check_vma=False
    )
```

```python
import functools
import math

import jax
import jax.numpy as jnp
from jax import lax
from jax.experimental import pallas as pl
from jax.experimental.pallas import tpu as pltpu
from jax.sharding import PartitionSpec as P

MESH = pl.DeviceIdType.MESH
F32, BF16, I32 = jnp.float32, jnp.bfloat16, jnp.int32
NZ, NP, NY, NX = 16, 8, 4, 4
HD, BLK, SUPER, NSEL, NFINE = 128, 128, 16, 4, 16
NREQ, SPAN = 512, 2048
NEG = -1e30
SCALE2 = HD**-0.5 / math.log(2.0)
Z_ORDER = (8, 7, 9, 6, 10, 5, 11, 4, 12, 3, 13, 2, 14, 1, 15)
PARTS = 1
NEAR = 4
PLANE = ((2, 0), (2, 1), (1, 0), (1, 1), (3, 0), (3, 1), (0, 1), (0, 0))


def iota(shape, dim):
    return lax.broadcasted_iota(I32, shape, dim)


def dot(a, b, dims=((1,), (0,))):
    return lax.dot_general(a, b, (dims, ((), ())), preferred_element_type=F32)


def group_rank(hits):
    i = jnp.bitwise_and(iota(hits[0].shape, 1), 3)
    before, total = [], []
    for h in hits:
        b = jnp.zeros_like(h)
        t = h
        for d in (1, 2, 3):
            b = b + jnp.where(i >= d, pltpu.roll(h, d, 1), 0)
            t = t + jnp.where(i + d <= 3, pltpu.roll(h, NREQ - d, 1), 0)
        before.append(b)
        total.append(t + b)
    return before[0], before[1] + total[0]


def kernel(
    q_h, kc_h, vc_h, sk_h, sv_h, om_h, si_h, fi_h, o_ref,
    sk, sv, om, si, fi, kcat, vcat, v_t, qz, qs, rq, rsel, meta, flag, pick, w_s,
    os_, ol, ro, rl, pzs, lzs, pz, lz, sz, szf, sf, xs,
    load_sem, kv_sem, q1s, q1r, q2s, q2r, r1s, r1r, l1s, l1r, r2s, r2r, l2s, l2r, szs, szr, sfs, sfr, xss, xsr, loc,
):
    me, rep = lax.axis_index("seq"), lax.axis_index("rep")
    z, p = me // NP, lax.rem(me, NP)
    y, c = p // 2, lax.rem(p, 2)

    def z_peer(d):
        return lax.rem(z + d, NZ)

    def plane_peer(dy, dc):
        return lax.rem(y + dy, NY) * 2 + lax.rem(c + dc, 2)

    plane = PLANE[:-1]

    barrier = pltpu.get_barrier_semaphore()
    for d in Z_ORDER:
        pl.semaphore_signal(barrier, inc=1, device_id=(z_peer(d) * NP + p, rep), device_id_type=MESH)
    for dy, dc in plane:
        pl.semaphore_signal(barrier, inc=1, device_id=(z * NP + plane_peer(dy, dc), rep), device_id_type=MESH)
    for d in range(1, NX):
        pl.semaphore_signal(barrier, inc=1, device_id=(me, lax.rem(rep + d, NX)), device_id_type=MESH)

    def remote(src, dst, ss, rs, seq, x=None):
        return pltpu.make_async_remote_copy(
            src_ref=src, dst_ref=dst, send_sem=ss, recv_sem=rs,
            device_id=(seq, rep if x is None else x), device_id_type=MESH,
        )

    def wait(ref, sem):
        pltpu.make_async_copy(ref, ref, sem).wait()

    loads = [
        pltpu.make_async_copy(a, b, load_sem.at[n])
        for n, (a, b) in enumerate([(q_h, qz.at[NEAR]), (sk_h, sk), (sv_h, sv), (om_h, om), (si_h, si), (fi_h, fi)])
    ]
    kv_loads = [
        pltpu.make_async_copy(a.at[g], b.at[:, pl.ds(g * HD, HD)], kv_sem.at[2 * n + g])
        for n, (a, b) in enumerate([(kc_h, kcat), (vc_h, vcat)])
        for g in (0, 1)
    ]
    for copy in loads + kv_loads:
        copy.start()
    for copy in loads:
        copy.wait()
    sz[z] = jnp.concatenate([sk[...].astype(F32), sv[...].astype(F32)], axis=0).astype(BF16)

    pl.semaphore_wait(barrier, len(Z_ORDER) + len(plane) + NX - 1)

    for d in Z_ORDER:
        e = (NEAR - d) % NZ
        remote(qz.at[NEAR], qz.at[e], q1s, q1r.at[e // 8], z_peer(d) * NP + p).start()

    omv = om[...]
    siv = [[si[g, j : j + 1, :] for j in range(NSEL)] for g in (0, 1)]
    lane128 = iota((NP, 128), 1)
    sig8 = jnp.sum(jnp.where(omv == z * NP + iota((NP, 128), 0), lane128, 0), axis=1, keepdims=True)
    hits = []
    for g in (0, 1):
        h = siv[g][0] == sig8
        for j in range(1, NSEL):
            h = jnp.logical_or(h, siv[g][j] == sig8)
        hits.append(jnp.where(h, 1, 0))
    ranks = group_rank(hits)
    row, lane = iota((NREQ, NREQ), 0), iota((NREQ, NREQ), 1)
    source = (((lane >> 5) + z + NZ - NEAR) & 15) * 32 + p * 4 + ((lane >> 3) & 3)
    picked = jnp.zeros((NP, NREQ), F32)
    for g in (0, 1):
        spread = jnp.where(row == jnp.where(((lane >> 2) & 1) == g, source, -1), 1.0, 0.0).astype(BF16)
        code = jnp.where(hits[g] > 0, ranks[g] + 1, 0).astype(F32).astype(BF16)
        picked = picked + dot(code, spread)
    rsel[...] = picked

    sig1 = jnp.sum(jnp.where(omv == me, lane128[0:1], 0), axis=1, keepdims=True)
    own_hits, own_bits = [], []
    for g in (0, 1):
        h, jsel = jnp.zeros((1, NREQ), I32), jnp.zeros((1, NREQ), I32)
        for j in range(NSEL):
            same = siv[g][j] == sig1
            h = jnp.where(same, 1, h)
            jsel = jnp.where(same, j, jsel)
        target = jsel * SUPER + iota((SUPER, NREQ), 0)
        bits = fi[g, 0:1, :] == target
        for k in range(1, NFINE):
            bits = jnp.logical_or(bits, fi[g, k : k + 1, :] == target)
        own_hits.append(jnp.broadcast_to(h, (8, NREQ)))
        own_bits.append(jnp.where(bits, 1.0, 0.0))
    own_ranks = group_rank(own_hits)
    sub8 = iota((8, NREQ), 0)
    stacked = []
    for slot in (0, 1):
        use = [jnp.where(jnp.logical_and(own_hits[g] > 0, own_ranks[g] == slot), 1.0, 0.0) for g in (0, 1)]
        wanted = own_bits[0] * use[0][0:1] + own_bits[1] * use[1][0:1]
        flags = jnp.where(sub8 == 0, use[0], jnp.where(sub8 == 1, use[1], 0.0))
        stacked.append(jnp.concatenate([wanted, flags, jnp.zeros((8, NREQ), F32)], axis=0).astype(BF16))
    for chunk in range(4):
        row, col = iota((NREQ, 256), 0), iota((NREQ, 256), 1)
        place = (chunk // 2) * 8 + ((col >> 3) & 7)
        chip = (y + NY - (chunk % 2) * 2 - (col >> 7)) & 3
        sender = ((place + z + NZ - NEAR) & 15) * NP + chip * 2 + ((col >> 6) & 1)
        acc = jnp.zeros((32, 256), F32)
        for slot in (0, 1):
            at = jnp.where(((col >> 2) & 1) == slot, sender, -1)
            acc = acc + dot(stacked[slot], jnp.where((row >> 2) == at, 1.0, 0.0).astype(BF16))
        meta[chunk] = acc
        flag[chunk] = jnp.transpose(acc[16:24], (1, 0))

    brow, blane = iota((32, 128), 0), iota((32, 128), 1)
    base = jnp.where(
        jnp.logical_and((brow >> 3) == (blane >> 5), (brow & 3) == (blane & 3)), ((brow >> 2) & 1) + 1, -1
    ).astype(F32)
    pick[...] = jnp.zeros_like(pick)
    w_s[...] = jnp.zeros_like(w_s)
    for n, (dy, dc) in enumerate(PLANE):
        code = rsel[pl.ds(plane_peer(dy, dc), 1), :]
        for b in range(4):
            same = base == code[:, b * 128 : (b + 1) * 128]
            at = (b // 2) * 512 + n * 64 + (b % 2) * 32
            pick[at : at + 32, (b % 2) * 128 : (b % 2) * 128 + 128] = jnp.where(same, 1.0, 0.0).astype(BF16)
    for copy in kv_loads:
        copy.wait()
    v_t[...] = jnp.transpose(vcat[...], (1, 0))

    for t in (0, 1):
        wait(qz.at[pl.ds(0, 7 + t)], q1r.at[t])
        every = qz[t * 8 : (t + 1) * 8].reshape(256, HD)
        rows = dot(pick[t * 512 : (t + 1) * 512, :], every).astype(BF16)
        qs[t] = rows.reshape(NP, 64, HD)
        for n, (dy, dc) in enumerate(PLANE):
            if dy or dc:
                remote(
                    qs.at[t, n], rq.at[t, dy * 2 + c], q2s, q2r.at[t, dy // 2], z * NP + plane_peer(dy, dc)
                ).start()
            else:
                pltpu.make_async_copy(qs.at[t, n], rq.at[t, c], loc.at[t]).start()
    for d in Z_ORDER:
        remote(sz.at[z], sz.at[z], szs, szr, z_peer(d) * NP + p).start()

    def batch_step(t, carry):
        wait(rq.at[0, 0], loc.at[t])
        wait(rq.at[0, pl.ds(0, 3)], q2r.at[t, 0])
        wait(rq.at[0, pl.ds(0, 4)], q2r.at[t, 1])
        m_all = jnp.concatenate([meta[t * 2], meta[t * 2 + 1]], axis=1)
        flags = jnp.concatenate([flag[t * 2], flag[t * 2 + 1]], axis=0).astype(BF16)
        rows = rq[t].reshape(NREQ, HD)
        split = jnp.concatenate([rows * flags[:, 0:1], rows * flags[:, 1:2]], axis=1)
        bias = jnp.where(m_all[0:16] > 0.5, 0.0, NEG)
        span, per = SPAN // PARTS, SUPER // PARTS
        outs, peaks, totals = [], [], []
        for g in range(PARTS):
            s = dot(kcat[g * span : (g + 1) * span, :], split, ((1,), (1,)))
            top = jnp.full((1, NREQ), -3e38, F32)
            for b in range(per):
                one = jnp.max(s[b * BLK : (b + 1) * BLK], axis=0, keepdims=True)
                top = jnp.maximum(top, one + bias[g * per + b : g * per + b + 1])
            part, ws = jnp.zeros((1, NREQ), F32), []
            for b in range(per):
                w = jnp.exp2((s[b * BLK : (b + 1) * BLK] + (bias[g * per + b : g * per + b + 1] - top)) * SCALE2)
                part = part + jnp.sum(w, axis=0, keepdims=True)
                ws.append(w.astype(BF16))
            outs.append(dot(v_t[:, g * span : (g + 1) * span], jnp.concatenate(ws, axis=0)))
            peaks.append(top)
            totals.append(part)
        peak = functools.reduce(jnp.maximum, peaks)
        factors = [jnp.exp2((top - peak) * SCALE2) for top in peaks]
        total = sum(f * part for f, part in zip(factors, totals))
        out = sum(f * o for f, o in zip(factors, outs))
        out = jnp.where(m_all[17:18] > 0.5, out[HD : 2 * HD], out[0:HD]) * (1.0 / total)
        out = jnp.transpose(out, (1, 0)).astype(BF16)
        os_[t] = out.reshape(NP, 64, HD)
        log_sum = peak * SCALE2 + jnp.log2(total)
        for a in range(NP):
            part = log_sum[:, (a // 2) * 128 : (a // 2) * 128 + 128]
            ol[t, a] = pltpu.roll(part, 64, 1) if a % 2 else part
        for k in (2, 1, 3):
            for core in (0, 1):
                peer = z * NP + lax.rem(y + NY - k, NY) * 2 + core
                remote(ol.at[t, k * 2 + core], rl.at[t, p], l1s, l1r.at[t], peer).start()
                remote(os_.at[t, k * 2 + core], ro.at[t, p], r1s, r1r.at[t], peer).start()
        remote(os_.at[t, 1 - c], ro.at[t, p], r1s, r1r.at[t], z * NP + y * 2 + 1 - c).start()
        remote(ol.at[t, 1 - c], rl.at[t, p], l1s, l1r.at[t], z * NP + y * 2 + 1 - c).start()
        pltpu.make_async_copy(os_.at[t, c], ro.at[t, p], loc.at[2 + t]).start()
        pltpu.make_async_copy(ol.at[t, c], rl.at[t, p], loc.at[4 + t]).start()
        return carry

    lax.fori_loop(0, 2, batch_step, 0)

    wait(sz.at[pl.ds(0, NZ - 1)], szr)
    for n in range(NZ):
        szf[n * 4 : n * 4 + 4, :] = sz[n].astype(F32)
    sf[p] = szf[...].astype(BF16)
    for dy, dc in plane:
        remote(sf.at[p], sf.at[p], sfs, sfr, z * NP + plane_peer(dy, dc)).start()

    keep = [
        pltpu.make_async_copy(pzs.at[NEAR], pz.at[z], loc.at[6]),
        pltpu.make_async_copy(lzs.at[NEAR], lz.at[z], loc.at[7]),
    ]
    for t in (0, 1):
        wait(os_.at[0, 0], loc.at[2 + t])
        wait(ol.at[0, 0], loc.at[4 + t])
        wait(rl.at[0, pl.ds(0, NP - 1)], l1r.at[t])
        l_cols = jnp.transpose(rl[t].reshape(NP, 128), (1, 0))
        for b in (0, 1):
            at = (t * 2 + b) * 128
            same = [base == rsel[n : n + 1, at : at + 128] for n in range(NP)]
            cols = l_cols[b * 32 : (b + 1) * 32]
            peak = jnp.full((32, 128), NEG, F32)
            for n in range(NP):
                peak = jnp.maximum(peak, jnp.where(same[n], cols[:, n : n + 1], NEG))
            peak = jnp.max(peak, axis=0, keepdims=True)
            ws = [jnp.where(same[n], jnp.exp2(cols[:, n : n + 1] - peak), 0.0) for n in range(NP)]
            total = jnp.sum(sum(ws), axis=0, keepdims=True)
            some = total > 0.0
            filled = jnp.where(some, total, 1.0)
            inverse = jnp.where(some, 1.0 / filled, 0.0)
            for n in range(NP):
                w_s[t, n * 64 + b * 32 : n * 64 + b * 32 + 32, b * 128 : (b + 1) * 128] = (ws[n] * inverse).astype(BF16)
            log_sum = jnp.where(some, peak + jnp.log2(filled), NEG)
            for k in range(4):
                lzs[t * 8 + b * 4 + k] = pltpu.roll(log_sum, 128 - 32 * k, 1) if k else log_sum
        for d in Z_ORDER:
            e = (d + NEAR) % NZ
            if e // 8 == t:
                remote(lzs.at[e], lz.at[z], l2s, l2r, z_peer(d) * NP + p).start()
        wait(ro.at[0, pl.ds(0, NP - 1)], r1r.at[t])
        merged = dot(w_s[t], ro[t].reshape(NREQ, HD), ((0,), (0,)))
        pzs[t * 8 : (t + 1) * 8] = merged.astype(BF16).reshape(8, 32, HD)
        if t == 0:
            for copy in keep:
                copy.start()
        for d in Z_ORDER:
            e = (d + NEAR) % NZ
            if e // 8 == t:
                remote(pzs.at[e], pz.at[z], r2s, r2r, z_peer(d) * NP + p).start()
    for copy in keep:
        copy.wait()

    wait(sf.at[pl.ds(0, NP - 1)], sfr)
    every_summary = sf[...].reshape(NREQ, HD)
    erow, elane = iota((128, 128), 0), iota((128, 128), 1)
    om_col = jnp.sum(jnp.where(erow == elane, omv, 0), axis=1, keepdims=True)
    tok = iota((1, NREQ), 1)
    tok_slot = ((tok >> 2) & 15) * NP + (tok >> 6)
    tok_super = jnp.sum(jnp.where(om_col == tok_slot, iota((128, NREQ), 0), 0), axis=0, keepdims=True)
    r_head, r_tok = iota((32, NREQ), 0), iota((32, NREQ), 1)
    r_group = (r_head >> 2) & 1
    kept = (r_tok & 3) == r_group
    for j in range(NSEL):
        ids = jnp.where(r_group == 0, siv[0][j], siv[1][j])
        own = jnp.sum(jnp.where(r_tok == me * 4 + (r_head >> 3), ids, 0), axis=1, keepdims=True)
        kept = jnp.logical_and(kept, tok_super != own)
    c_score = dot(qz[NEAR], every_summary, ((1,), (1,))) * SCALE2 + 4.0
    c_score = jnp.where(kept, c_score, NEG)
    c_peak = jnp.max(c_score, axis=1, keepdims=True)
    c_w = jnp.where(kept, jnp.exp2(c_score - c_peak), 0.0)
    c_sum = jnp.sum(c_w, axis=1, keepdims=True)
    c_out = dot(pltpu.roll(c_w, 2, 1).astype(BF16), every_summary)

    wait(pz.at[pl.ds(0, NZ - 1)], r2r)
    wait(lz.at[pl.ds(0, NZ - 1)], l2r)

    lse = jnp.transpose(lz[...].reshape(NZ, 128), (1, 0))[0:32]
    c_lse = c_peak + jnp.log2(c_sum)
    top = jnp.maximum(jnp.max(lse, axis=1, keepdims=True), c_lse)
    w = jnp.exp2(lse - top)
    c_scale = jnp.exp2(c_peak - top)
    total = jnp.sum(w, axis=1, keepdims=True) + c_scale * c_sum
    result = c_out * c_scale
    for n in range(NZ):
        result = result + pz[n].astype(F32) * w[:, n : n + 1]
    xs[...] = (result / total).astype(BF16).reshape(NX, 8, HD)
    keep = pltpu.make_async_copy(xs.at[rep], o_ref.at[rep], loc.at[8])
    keep.start()
    for d in range(1, NX):
        x = lax.rem(rep + d, NX)
        remote(xs.at[x], o_ref.at[rep], xss, xsr, me, x).start()

    wait(qz.at[pl.ds(0, NZ - 1)], q1s)
    wait(sz.at[pl.ds(0, NZ - 1)], szs)
    for t in (0, 1):
        wait(qs.at[t, pl.ds(0, NP - 1)], q2s)
    wait(sf.at[pl.ds(0, NP - 1)], sfs)
    for t in (0, 1):
        wait(os_.at[t, pl.ds(0, NP - 1)], r1s)
        wait(ol.at[t, pl.ds(0, NP - 1)], l1s)
    wait(pzs.at[pl.ds(0, NZ - 1)], r2s)
    wait(lzs.at[pl.ds(0, NZ - 1)], l2s)
    keep.wait()
    wait(xs.at[pl.ds(0, NX - 1)], xss)
    wait(o_ref.at[pl.ds(0, NX - 1)], xsr)


def shards(queries, key_cache, value_cache, summary_keys, summary_values, owner_map, super_ids, fine_ids):
    vmem, dma = pltpu.VMEM, pltpu.SemaphoreType.DMA
    out = pl.pallas_call(
        kernel,
        out_shape=jax.ShapeDtypeStruct((NX, 8, HD), BF16),
        in_specs=[pl.BlockSpec(memory_space=pltpu.HBM)] * 8,
        out_specs=pl.BlockSpec(memory_space=pltpu.HBM),
        scratch_shapes=[
            vmem((2, HD), BF16),
            vmem((2, HD), BF16),
            vmem((1, 128), I32),
            vmem((2, NSEL, NREQ), I32),
            vmem((2, NFINE, NREQ), I32),
            vmem((SPAN, 2 * HD), BF16),
            vmem((SPAN, 2 * HD), BF16),
            vmem((2 * HD, SPAN), BF16),
            vmem((NZ, 32, HD), BF16),
            vmem((2, NP, 64, HD), BF16),
            vmem((2, NP, 64, HD), BF16),
            vmem((NP, NREQ), F32),
            vmem((4, 32, 256), F32),
            vmem((4, 256, 8), F32),
            vmem((2 * NREQ, 256), BF16),
            vmem((2, NREQ, 256), BF16),
            vmem((2, NP, 64, HD), BF16),
            vmem((2, NP, 1, 128), F32),
            vmem((2, NP, 64, HD), BF16),
            vmem((2, NP, 1, 128), F32),
            vmem((NZ, 32, HD), BF16),
            vmem((NZ, 1, 128), F32),
            vmem((NZ, 32, HD), BF16),
            vmem((NZ, 1, 128), F32),
            vmem((NZ, 4, HD), BF16),
            vmem((NZ * 4, HD), F32),
            vmem((NP, NZ * 4, HD), BF16),
            vmem((NX, 8, HD), BF16),
            dma((6,)),
            dma((4,)),
            dma,
            dma((2,)),
            dma,
            dma((2, 2)),
            dma,
            dma((2,)),
            dma,
            dma((2,)),
        ]
        + [dma] * 10
        + [dma((9,))],
        compiler_params=pltpu.CompilerParams(collective_id=0, has_side_effects=True),
    )(
        queries.reshape(32, HD),
        key_cache,
        value_cache,
        summary_keys.reshape(2, HD),
        summary_values.reshape(2, HD),
        owner_map.reshape(1, 128),
        jnp.transpose(super_ids, (1, 2, 0)),
        jnp.transpose(fine_ids, (1, 2, 0)),
    )
    return out.reshape(1, NX * 8, HD)


def solution(mesh):
    in_specs = (
        P("seq", "rep", None),
        P("rep", "seq", None),
        P("rep", "seq", None),
        P("rep", "seq", None),
        P("rep", "seq", None),
        P(),
        P(None, "rep", None),
        P(None, "rep", None),
    )
    return jax.shard_map(
        shards, mesh=mesh, in_specs=in_specs, out_specs=P(("seq", "rep"), None, None), check_vma=False
    )
```
